8 devices in a mesh: dp: 2 (over z, y), tp: 4 (over x, core).
Axes of the slice: x: 2, y: 2, z: 1, core: 2. Of those that a mesh axis runs over, the one named last changes fastest.
Arguments:
- x: bfloat16 [16384, 2048], P(('dp', 'tp'))
- grad_y: bfloat16 [16384, 2048], P(('dp', 'tp'))
- ln_gain: float32 [2048], replicated
- positions: int32 [1024], replicated
- w_q: bfloat16 [2048, 2048], P('dp', 'tp')
- w_kv: bfloat16 [2048, 512], P('dp')
- w_o: bfloat16 [2048, 2048], P('tp', 'dp')
- w_in: bfloat16 [2, 2048, 16384], P(None, 'dp', 'tp')
- w_out: bfloat16 [16384, 2048], P('tp', 'dp')
Outputs:
- output 1: bfloat16 [16384, 2048], P(('dp', 'tp'))
- output 2: bfloat16 [16384, 2048], P(('dp', 'tp'))
- output 3: bfloat16 [2048, 2048], P('dp', 'tp')
- output 4: bfloat16 [2048, 512], P('dp')
- output 5: bfloat16 [2048, 2048], P('tp', 'dp')
- output 6: bfloat16 [2, 2048, 16384], P(None, 'dp', 'tp')
- output 7: bfloat16 [16384, 2048], P('tp', 'dp')
All inputs are finite; a program needn't handle non-finite values.
Results may differ from the reference program's by a relative error of at most 0.0126665.
Values are sent between devices in bfloat16 or wider.
A program may use at most 1 GiB of HBM per device.

```python
import jax
import jax.numpy as jnp
from jax import lax

D_MODEL = 2048
HEADS = 8
HEAD_DIM = 256
FF_DIM = 16384
SEQ_LEN = 1024
NUM_SEQS = 16
TOKENS = NUM_SEQS * SEQ_LEN
LN_EPS = 1e-6


def setup_inputs(seed: int = 0) -> dict:
    rand_keys = jax.random.split(jax.random.key(seed), 9)
    x = jax.random.normal(rand_keys[0], (TOKENS, D_MODEL), jnp.float32)
    grad_y = jax.random.normal(rand_keys[1], (TOKENS, D_MODEL), jnp.float32)
    ln_gain = 1.0 + 0.3 * jax.random.normal(rand_keys[2], (D_MODEL,), jnp.float32)
    positions = jax.random.permutation(rand_keys[3], SEQ_LEN).astype(jnp.int32)
    w_q = jax.random.normal(rand_keys[4], (D_MODEL, HEADS * HEAD_DIM), jnp.float32) * D_MODEL ** -0.5
    w_kv = jax.random.normal(rand_keys[5], (D_MODEL, 2 * HEAD_DIM), jnp.float32) * D_MODEL ** -0.5
    w_o = jax.random.normal(rand_keys[6], (HEADS * HEAD_DIM, D_MODEL), jnp.float32) * (HEADS * HEAD_DIM) ** -0.5
    w_in = jax.random.normal(rand_keys[7], (2, D_MODEL, FF_DIM), jnp.float32) * D_MODEL ** -0.5
    w_out = jax.random.normal(rand_keys[8], (FF_DIM, D_MODEL), jnp.float32) * FF_DIM ** -0.5
    return {"x": x.astype(jnp.bfloat16), "grad_y": grad_y.astype(jnp.bfloat16), "ln_gain": ln_gain, "positions": positions, "w_q": w_q.astype(jnp.bfloat16), "w_kv": w_kv.astype(jnp.bfloat16), "w_o": w_o.astype(jnp.bfloat16), "w_in": w_in.astype(jnp.bfloat16), "w_out": w_out.astype(jnp.bfloat16)}


def normalize(x_rows, ln_gain):
    x_wide = x_rows.astype(jnp.float32)
    centered = x_wide - jnp.mean(x_wide, axis=-1, keepdims=True)
    variance = jnp.mean(centered * centered, axis=-1, keepdims=True)
    return centered * lax.rsqrt(variance + LN_EPS) * ln_gain


def block_forward(x, ln_gain, positions, w_q, w_kv, w_o, w_in, w_out):
    normed_wide = normalize(x, ln_gain)
    q_proj = jnp.dot(normed_wide.astype(jnp.bfloat16), w_q, preferred_element_type=jnp.float32).astype(jnp.bfloat16)
    kv_proj = jnp.dot(normed_wide.astype(jnp.bfloat16), w_kv, preferred_element_type=jnp.float32).astype(jnp.bfloat16)
    gate_proj = jnp.dot(normed_wide.astype(jnp.bfloat16), w_in[0], preferred_element_type=jnp.float32).astype(jnp.bfloat16)
    up_proj = jnp.dot(normed_wide.astype(jnp.bfloat16), w_in[1], preferred_element_type=jnp.float32).astype(jnp.bfloat16)
    q_seq = q_proj.reshape(NUM_SEQS, SEQ_LEN, HEADS, HEAD_DIM)
    key_seq = kv_proj[:, :HEAD_DIM].reshape(NUM_SEQS, SEQ_LEN, HEAD_DIM)
    val_seq = kv_proj[:, HEAD_DIM:].reshape(NUM_SEQS, SEQ_LEN, HEAD_DIM)
    visible = positions[None, :] <= positions[:, None]

    def attend_one(operands):
        q_one, k_one, v_one = operands
        scores = jnp.einsum("qhe,ke->hqk", q_one.astype(jnp.float32), k_one.astype(jnp.float32)) * HEAD_DIM ** -0.5
        scores = jnp.where(visible[None], scores, -1e30)
        attn_prob = jax.nn.softmax(scores, axis=-1).astype(jnp.bfloat16)
        attn_out = jnp.einsum("hqk,ke->qhe", attn_prob.astype(jnp.float32), v_one.astype(jnp.float32))
        return attn_out.astype(jnp.bfloat16)

    attn_heads = lax.map(jax.checkpoint(attend_one), (q_seq, key_seq, val_seq))
    attn_heads = attn_heads.reshape(TOKENS, HEADS * HEAD_DIM)
    swiglu_out = (jax.nn.silu(gate_proj.astype(jnp.float32)) * up_proj.astype(jnp.float32)).astype(jnp.bfloat16)
    branch_sum = jnp.dot(attn_heads, w_o, preferred_element_type=jnp.float32) + jnp.dot(swiglu_out, w_out, preferred_element_type=jnp.float32)
    return branch_sum.astype(jnp.bfloat16)


def reference(x, grad_y, ln_gain, positions, w_q, w_kv, w_o, w_in, w_out):
    def with_weights(x_in, wq_in, wkv_in, wo_in, win_in, wout_in):
        return block_forward(x_in, ln_gain, positions, wq_in, wkv_in, wo_in, win_in, wout_in)

    y_out, pullback = jax.vjp(with_weights, x, w_q, w_kv, w_o, w_in, w_out)
    grad_x, grad_w_q, grad_w_kv, grad_w_o, grad_w_in, grad_w_out = pullback(grad_y)
    return (y_out, grad_x, grad_w_q, grad_w_kv, grad_w_o, grad_w_in, grad_w_out)
```

```python
import functools

import jax
import jax.numpy as jnp
from jax import lax
from jax.experimental import pallas as pl
from jax.experimental.pallas import tpu as pltpu
from jax.sharding import PartitionSpec as P


LN_EPS = 1e-6
MASK_FILL = -1e30
BF16 = jnp.bfloat16
F32 = jnp.float32
NN = (((1,), (0,)), ((), ()))
NT = (((1,), (1,)), ((), ()))
TN = (((0,), (0,)), ((), ()))
VMEM_LIMIT = 60 << 20
CHUNKS = 4


def mm(lhs, rhs, dims):
    return lax.dot_general(lhs, rhs, dims, preferred_element_type=F32)


def hidden(n):
    return [pl.BlockSpec(memory_space=pl.ANY)] * n


def params(n_axes):
    return pltpu.CompilerParams(dimension_semantics=("arbitrary",) * n_axes, vmem_limit_bytes=VMEM_LIMIT)


def norm_kernel(x_ref, gain_ref, h_ref):
    x = x_ref[...].astype(F32)
    c = x - jnp.mean(x, axis=-1, keepdims=True)
    var = jnp.mean(c * c, axis=-1, keepdims=True)
    h_ref[...] = (c * lax.rsqrt(var + LN_EPS) * gain_ref[...]).astype(BF16)


def norm_grad_kernel(x_ref, gain_ref, dh_ref, dx_ref):
    x = x_ref[...].astype(F32)
    c = x - jnp.mean(x, axis=-1, keepdims=True)
    rstd = lax.rsqrt(jnp.mean(c * c, axis=-1, keepdims=True) + LN_EPS)
    unit = c * rstd
    d = dh_ref[...].astype(F32) * gain_ref[...]
    d_mean = jnp.mean(d, axis=-1, keepdims=True)
    d_unit = jnp.mean(d * unit, axis=-1, keepdims=True)
    dx_ref[...] = (rstd * (d - d_mean - unit * d_unit)).astype(BF16)


def row_call(kernel, gain, *rows):
    tokens, width = rows[0].shape
    tm = min(256, tokens)
    block = pl.BlockSpec((tm, width), lambda m: (m, 0))
    return pl.pallas_call(
        kernel,
        grid=(tokens // tm,),
        in_specs=[block, pl.BlockSpec((1, width), lambda m: (0, 0))] + [block] * (len(rows) - 1),
        out_specs=block,
        out_shape=jax.ShapeDtypeStruct((tokens, width), BF16),
        compiler_params=params(1),
        cost_estimate=pl.CostEstimate(flops=16 * tokens * width, bytes_accessed=2 * tokens * width * (len(rows) + 1), transcendentals=tokens),
    )(rows[0], gain[None, :], *rows[1:])


def attention_kernel(scale, pos_q_ref, pos_k_ref, q_ref, key_ref, val_ref, do_ref, *rest):
    o_ref, dq_ref, dkv_ref = rest[-3:]
    head_dim = q_ref.shape[-1]
    visible = pos_k_ref[...] <= pos_q_ref[...]
    q, k, v, do = q_ref[...], key_ref[...], val_ref[...], do_ref[...]
    s = jnp.where(visible, mm(q, k, NT) * scale, MASK_FILL)
    e = jnp.exp(s - jnp.max(s, axis=-1, keepdims=True))
    p = (e / jnp.sum(e, axis=-1, keepdims=True)).astype(BF16)
    o_ref[...] = mm(p, v, NN).astype(BF16)
    dp = mm(do, v, NT).astype(BF16).astype(F32)
    pw = p.astype(F32)
    dot = jnp.sum(pw * dp, axis=-1, keepdims=True)
    ds = (pw * (dp - dot) * scale).astype(BF16)
    dq_ref[...] = mm(ds, k, NN).astype(BF16)

    @pl.when(pl.program_id(1) == 0)
    def _():
        dkv_ref[:, :head_dim] = mm(ds, q, TN)
        dkv_ref[:, head_dim:] = mm(p, do, TN)

    @pl.when(pl.program_id(1) > 0)
    def _():
        dkv_ref[:, :head_dim] += mm(ds, q, TN)
        dkv_ref[:, head_dim:] += mm(p, do, TN)


def attention(q, kv, do, positions, head_dim, after=()):
    tokens, width = q.shape
    seq = positions.shape[0]
    heads = width // head_dim
    block = lambda f: pl.BlockSpec((seq, head_dim), f)
    return pl.pallas_call(
        functools.partial(attention_kernel, head_dim ** -0.5),
        grid=(tokens // seq, heads),
        in_specs=[
            pl.BlockSpec((seq, 1), lambda s, h: (0, 0)),
            pl.BlockSpec((1, seq), lambda s, h: (0, 0)),
            block(lambda s, h: (s, h)),
            block(lambda s, h: (s, 0)),
            block(lambda s, h: (s, 1)),
            block(lambda s, h: (s, h)),
        ] + hidden(len(after)),
        out_specs=[block(lambda s, h: (s, h)), block(lambda s, h: (s, h)), pl.BlockSpec((seq, 2 * head_dim), lambda s, h: (s, 0))],
        out_shape=[
            jax.ShapeDtypeStruct((tokens, width), BF16),
            jax.ShapeDtypeStruct((tokens, width), BF16),
            jax.ShapeDtypeStruct((tokens, 2 * head_dim), F32),
        ],
        compiler_params=params(2),
        cost_estimate=pl.CostEstimate(flops=20 * tokens * seq * width, bytes_accessed=tokens * width * 14, transcendentals=tokens * seq * heads),
        name="attention",
    )(positions[:, None], positions[None, :], q, kv, kv, do, *after)


def mlp_kernel(sub, h_ref, gy_ref, win_ref, wout_ref, *rest):
    a_ref, dg_ref, du_ref = rest[-3:]
    for c in range(0, a_ref.shape[-1], sub):
        cols = slice(c, c + sub)
        g = mm(h_ref[...], win_ref[0, :, cols], NN).astype(BF16).astype(F32)
        u = mm(h_ref[...], win_ref[1, :, cols], NN).astype(BF16).astype(F32)
        d = mm(gy_ref[...], wout_ref[cols, :], NT).astype(BF16).astype(F32)
        sig = jax.nn.sigmoid(g)
        silu = g * sig
        a_ref[:, cols] = (silu * u).astype(BF16)
        du_ref[:, cols] = (d * silu).astype(BF16)
        dg_ref[:, cols] = (d * u * (sig + silu * (1.0 - sig))).astype(BF16)


def mlp_chunk(h, gy, win, wout, after=()):
    tokens, d_model = h.shape
    cols = wout.shape[0]
    tm, tn = min(512, tokens), min(512, cols)
    out_block = pl.BlockSpec((tm, tn), lambda n, m: (m, n))
    return pl.pallas_call(
        functools.partial(mlp_kernel, min(256, tn)),
        grid=(cols // tn, tokens // tm),
        in_specs=[
            pl.BlockSpec((tm, d_model), lambda n, m: (m, 0)),
            pl.BlockSpec((tm, d_model), lambda n, m: (m, 0)),
            pl.BlockSpec((2, d_model, tn), lambda n, m: (0, 0, n)),
            pl.BlockSpec((tn, d_model), lambda n, m: (n, 0)),
        ] + hidden(len(after)),
        out_specs=[out_block] * 3,
        out_shape=[jax.ShapeDtypeStruct((tokens, cols), BF16)] * 3,
        compiler_params=params(2),
        cost_estimate=pl.CostEstimate(flops=6 * tokens * d_model * cols, bytes_accessed=4 * tokens * d_model * (cols // tn) + 6 * tokens * cols, transcendentals=tokens * cols),
        name="mlp_chunk",
    )(h, gy, win, wout, *after)


def sum_kernel(terms, n_in, n_adds, out_dtype, *refs):
    out_ref = refs[-1]
    acc = None
    for lhs, rhs, pick, dims in terms:
        right = refs[rhs][...] if pick is None else refs[rhs][pick]
        part = mm(refs[lhs][...], right, dims)
        acc = part if acc is None else acc + part
    for i in range(n_in, n_in + n_adds):
        acc = acc + refs[i][...]
    out_ref[...] = acc.astype(out_dtype)


def sum_rows(products, adds, row0, rows, width, out_dtype, tm, tn, after=()):
    tm, tn = min(tm, rows), min(tn, width)
    base = row0 // tm
    arrays, specs, terms = [], [], []
    k_total = 0
    for lhs, rhs, form in products:
        left = lhs if isinstance(lhs, tuple) else (lhs,)
        first = len(arrays)
        for part in left:
            arrays.append(part)
            offset = base if part.shape[0] > rows else 0
            specs.append(pl.BlockSpec((tm, part.shape[1]), lambda n, m, o=offset: (o + m, 0)))
            k_total += part.shape[1]
        at = len(arrays)
        arrays.append(rhs)
        if form == "n":
            specs.append(pl.BlockSpec((rhs.shape[0], tn), lambda n, m: (0, n)))
        elif rhs.ndim == 2:
            specs.append(pl.BlockSpec((tn, rhs.shape[1]), lambda n, m: (n, 0)))
        else:
            specs.append(pl.BlockSpec((rhs.shape[0], tn, rhs.shape[2]), lambda n, m: (0, n, 0)))
        for i in range(len(left)):
            terms.append((first + i, at, i if rhs.ndim == 3 else None, NN if form == "n" else NT))
    n_in = len(arrays)
    for add in adds:
        arrays.append(add)
        specs.append(pl.BlockSpec((tm, tn), lambda n, m: (m, n)))
    return pl.pallas_call(
        functools.partial(sum_kernel, tuple(terms), n_in, len(adds), out_dtype),
        grid=(width // tn, rows // tm),
        in_specs=specs + hidden(len(after)),
        out_specs=pl.BlockSpec((tm, tn), lambda n, m: (m, n)),
        out_shape=jax.ShapeDtypeStruct((rows, width), out_dtype),
        compiler_params=params(2),
        cost_estimate=pl.CostEstimate(flops=2 * rows * width * k_total, bytes_accessed=2 * rows * k_total * (width // tn) + 2 * width * k_total + 4 * rows * width * (1 + len(adds)), transcendentals=0),
    )(*arrays, *after)


def pair_kernel(half, first_ref, second_ref, *rest):
    out_ref = rest[-1]

    @pl.when(pl.program_id(0) < half)
    def _():
        out_ref[...] = first_ref[...]

    @pl.when(pl.program_id(0) >= half)
    def _():
        out_ref[...] = second_ref[...]


def pair(first, second, after=()):
    tokens, width = first.shape
    tm = min(512, tokens)
    half = tokens // tm
    return pl.pallas_call(
        functools.partial(pair_kernel, half),
        grid=(2 * half,),
        in_specs=[
            pl.BlockSpec((tm, width), lambda m: (jnp.minimum(m, half - 1), 0)),
            pl.BlockSpec((tm, width), lambda m: (jnp.maximum(m - half, 0), 0)),
        ] + hidden(len(after)),
        out_specs=pl.BlockSpec((tm, width), lambda m: (m, 0)),
        out_shape=jax.ShapeDtypeStruct((2 * tokens, width), first.dtype),
        compiler_params=params(1),
        cost_estimate=pl.CostEstimate(flops=tokens * width, bytes_accessed=8 * tokens * width, transcendentals=0),
        name="pair",
    )(first, second, *after)


def place_kernel(piece_ref, *rest):
    rest[-1][...] = piece_ref[...].astype(BF16)


def place(piece, buffer, shape, index):
    dims = piece.shape
    rows = min(256, dims[0])
    lead = (1,) * (len(shape) - 2)
    at = lambda m: index[:-2] + (index[-2] * (dims[0] // rows) + m, index[-1])
    carried = () if buffer is None else (buffer,)
    return pl.pallas_call(
        place_kernel,
        grid=(dims[0] // rows,),
        in_specs=[pl.BlockSpec((rows, dims[1]), lambda m: (m, 0))] + hidden(len(carried)),
        out_specs=pl.BlockSpec((None,) * len(lead) + (rows, dims[1]), at),
        out_shape=jax.ShapeDtypeStruct(shape, BF16),
        input_output_aliases={1: 0} if carried else {},
        compiler_params=params(1),
        cost_estimate=pl.CostEstimate(flops=dims[0] * dims[1], bytes_accessed=6 * dims[0] * dims[1], transcendentals=0),
        name="place",
    )(piece, *carried)


def solution(mesh):
    tp = mesh.shape["tp"]
    row_spec = P(("dp", "tp"), None)
    weight_specs = (P("dp", "tp"), P("dp", None), P("tp", "dp"), P(None, "dp", "tp"), P("tp", "dp"))
    core_pairs = [(i, i ^ 1) for i in range(tp)]
    chip_pairs = [(i, i ^ 2) for i in range(tp)]

    def core(v):
        return lax.ppermute(v, "tp", core_pairs)

    def across(v):
        return lax.ppermute(v, "tp", chip_pairs)

    def tied(v, after):
        return lax.optimization_barrier((v, after))[0]

    def device_body(x_rows, gy_rows, ln_gain, positions, wq_shard, wkv_shard, wo_shard, win_shard, wout_shard):
        head_dim = wkv_shard.shape[1] // 2
        block, d_model = x_rows.shape
        ff = wout_shard.shape[0]
        step = ff // CHUNKS
        tp_index = lax.axis_index("tp")
        on_core, on_chip = tp_index % 2, tp_index // 2

        normed = row_call(norm_kernel, ln_gain, x_rows)
        h_across = across(normed)
        gy_across = across(gy_rows)
        h_near = pair(normed, core(normed))
        gy_near = pair(gy_rows, core(gy_rows))

        w_kv = lax.all_gather(wkv_shard, "dp", axis=0, tiled=True)
        w_q = lax.all_gather(wq_shard, "dp", axis=0, tiled=True)
        w_o = lax.all_gather(wo_shard, "dp", axis=1, tiled=True)
        win_late, wout_late = tied((win_shard, wout_shard), normed)
        w_in, w_out = [], []
        for j in range(CHUNKS):
            w_in.append(lax.all_gather(win_late[:, :, j * step:(j + 1) * step], "dp", axis=1, tiled=True))
            w_out.append(lax.all_gather(wout_late[j * step:(j + 1) * step], "dp", axis=1, tiled=True))

        def attend(h, gy):
            kv = mm(h, w_kv, NN).astype(BF16)
            q = mm(h, w_q, NN).astype(BF16)
            do = mm(gy, w_o, NT).astype(BF16)
            return attention(q, kv, do, positions, head_dim)

        o_near, dq_near, dkv_near = attend(h_near, gy_near)
        acts_near = [mlp_chunk(h_near, gy_near, w_in[0], w_out[0], after=(o_near,))]
        h_far = pair(h_across, core(h_across), after=(acts_near[0][0],))
        gy_far = pair(gy_across, core(gy_across), after=(acts_near[0][0],))
        o_far, dq_far, dkv_far = attend(h_far, gy_far)
        acts_far = [mlp_chunk(h_far, gy_far, w_in[0], w_out[0], after=(o_far,))]
        last = acts_far[0][0]

        from_core = core(dkv_near[block:]), core(dkv_far[block:])
        dkv_own = dkv_near[:block] + from_core[0]
        dkv_other = dkv_far[:block] + from_core[1]
        dkv_from = across(dkv_other)
        d_kv = (dkv_own + dkv_from).astype(BF16)

        def weight_grad(left, right, axis, last):
            parts = [mm(tied(left[i], last), right[i], TN) for i in range(2)]
            part = parts[0] + parts[1]
            return part, lax.psum_scatter(part, "dp", scatter_dimension=axis, tiled=True)

        h_both, gy_both = (h_near, h_far), (gy_near, gy_far)
        grad_out, grad_in = [None] * CHUNKS, [[None] * CHUNKS, [None] * CHUNKS]

        def do_out(j, last):
            part, grad_out[j] = weight_grad((acts_near[j][0], acts_far[j][0]), gy_both, 1, last)
            return part

        def do_in(j, last):
            for g in range(2):
                last, grad_in[g][j] = weight_grad(h_both, (acts_near[j][1 + g], acts_far[j][1 + g]), 0, last)
            return last

        def do_act(j, last):
            acts_near.append(mlp_chunk(h_near, gy_near, w_in[j], w_out[j], after=(last,)))
            acts_far.append(mlp_chunk(h_far, gy_far, w_in[j], w_out[j], after=(acts_near[-1][0],)))
            return acts_far[-1][0]

        def y_rows(near, row0, adds, dtype, last):
            acts, o = (acts_near, o_near) if near else (acts_far, o_far)
            products = [(acts[j][0], w_out[j], "n") for j in range(CHUNKS)] + [(o, w_o, "n")]
            return sum_rows(products, adds, row0, block, d_model, dtype, 512, 1024, after=(last,))

        def dh_rows(near, row0, adds, dtype, last, more=()):
            acts, dq = (acts_near, dq_near) if near else (acts_far, dq_far)
            products = [((acts[j][1], acts[j][2]), w_in[j], "t") for j in range(CHUNKS)] + [(dq, w_q, "t"), *more]
            return sum_rows(products, adds, row0, block, d_model, dtype, 512, 512, after=(last,))

        last, grad_wq = weight_grad(h_both, (dq_near, dq_far), 0, last)
        last, grad_wo = weight_grad((o_near, o_far), gy_both, 1, last)
        last = do_out(0, last)

        pick = lambda v, at: lax.dynamic_slice_in_dim(v, at * (v.shape[1] // 2), v.shape[1] // 2, axis=1)
        last = wkv_part = mm(tied(normed, last), d_kv, TN)
        wkv_part = pick(wkv_part, on_core) + core(pick(wkv_part, 1 - on_core))
        wkv_part = pick(wkv_part, on_chip) + across(pick(wkv_part, 1 - on_chip))
        last = do_in(0, last)
        last = do_act(1, last)
        last = do_out(1, last)
        last = do_act(2, last)
        last = do_in(1, last)
        last = do_act(3, last)
        y_diag = y_rows(False, block, (), F32, last)
        y_diag_from = core(y_diag)
        last = do_out(2, y_diag)
        grad_wkv = lax.psum_scatter(tied(wkv_part, last), "dp", scatter_dimension=0, tiled=True).astype(BF16)
        for exchange, side in ((across, on_chip), (core, on_core)):
            other = exchange(grad_wkv)
            grad_wkv = jnp.where(side == 0, jnp.concatenate([grad_wkv, other], axis=1), jnp.concatenate([other, grad_wkv], axis=1))

        y_across = y_rows(False, 0, (y_diag_from,), F32, last)
        y_from = across(y_across)
        last = do_in(2, y_across)
        dh_diag = dh_rows(False, block, (), F32, last)
        dh_diag_from = core(dh_diag)
        last = do_out(3, dh_diag)
        dh_across = dh_rows(False, 0, (dh_diag_from,), F32, last)
        dh_from = across(dh_across)
        last = do_in(3, dh_across)
        y_core = y_rows(True, block, (), F32, last)
        y_core_from = core(y_core)
        dh_core = dh_rows(True, block, (), F32, y_core)
        dh_core_from = core(dh_core)
        y_own = y_rows(True, 0, (y_core_from, y_from), BF16, dh_core)
        dh_own = dh_rows(True, 0, (dh_core_from, dh_from), BF16, y_own, more=((d_kv, w_kv, "t"),))
        grad_x = row_call(norm_grad_kernel, ln_gain, x_rows, dh_own)

        win_grad = wout_grad = None
        for j in range(CHUNKS):
            wout_grad = place(grad_out[j], wout_grad, wout_shard.shape, (j, 0))
            for g in range(2):
                win_grad = place(grad_in[g][j], win_grad, win_shard.shape, (g, 0, j))
        return y_own, grad_x, grad_wq.astype(BF16), grad_wkv, grad_wo.astype(BF16), win_grad, wout_grad

    return jax.shard_map(device_body, mesh=mesh, in_specs=(row_spec, row_spec, P(None), P(None)) + weight_specs, out_specs=(row_spec, row_spec) + weight_specs, check_vma=False)
```
